32 devices in a mesh: ep: 4 (over z), fsdp: 8 (over y, x, core).
Axes of the slice: x: 2, y: 2, z: 4, core: 2. Of those that a mesh axis runs over, the one named last changes fastest.
Arguments:
- train_gate: float32 [64, 2048, 1408], P('ep', 'fsdp'), may hold values from -0.1875 to 0.1875
- train_up: float32 [64, 2048, 1408], P('ep', 'fsdp'), may hold values from -0.1875 to 0.1875
- train_down: float32 [64, 1408, 2048], P('ep', None, 'fsdp'), may hold values from -0.21875 to 0.21875
- router_weight: float32 [2048, 64], P('fsdp', 'ep'), may hold values from -0.125 to 0.125
- router_gain: float32 [2048], P('fsdp'), may hold values from 0.25 to 1.75
Outputs:
- ready_gate: bfloat16 [64, 2048, 1408], P('ep', None, 'fsdp')
- ready_up: bfloat16 [64, 2048, 1408], P('ep', None, 'fsdp')
- ready_down: bfloat16 [64, 1408, 2048], P('ep', 'fsdp')
- scale_gate: float32 [64, 1408], P('ep', 'fsdp')
- scale_up: float32 [64, 1408], P('ep', 'fsdp')
- scale_down: float32 [64, 1408], P('ep', 'fsdp')
- serve_router: bfloat16 [2048, 64], replicated
The draws below stay inside these ranges and needn't reach their ends.
All inputs are finite; a program needn't handle non-finite values. Where the reference program divides by a largest or mean magnitude, that divisor is 1e-20 or more.
Results may differ from the reference program's by a relative error of at most 0.012.
Values may be sent and summed in bfloat16 or wider, within the bound.
A program may use at most 192 MiB of HBM per device.

```python
import jax
import jax.numpy as jnp

EXPERTS = 64
D_MODEL = 2048
D_EXPERT = 1408


def spiked(array, key, source, target, parts, factor):
    owner, partner = [(jnp.arange(array.shape[axis_at]) // (array.shape[axis_at] // parts)).reshape([-1 if axis == axis_at else 1 for axis in range(array.ndim)]) for axis_at in (source, target)]
    chosen = jax.random.permutation(key, parts)[partner]
    strong = (owner == chosen) | (owner == (partner + parts // 2) % parts)
    return jnp.where(strong, factor * array, array)


def block_levels(rng, extent, cuts, smallest, high):
    loudness = 1.0
    for axis_at, shards_of in cuts:
        heights = jax.random.uniform(jax.random.fold_in(jax.random.fold_in(rng, 6), axis_at), (shards_of,), jnp.float32, smallest / len(cuts), high / len(cuts))
        loudness = loudness * jnp.repeat(jnp.exp(heights), extent[axis_at] // shards_of).reshape((-1,) + (1,) * (len(extent) - 1 - axis_at))
    return loudness


def scatter_about(rng, shape, spread, reach, split=(), dtype=jnp.bfloat16):
    drawn = spread * jax.random.normal(rng, shape, jnp.float32)
    if split:
        drawn = drawn * block_levels(rng, shape, split, -0.22, 0.18)
    return jnp.clip(drawn, -reach, reach).astype(dtype)


def bell_draw_with(key, shape, spread, bound, pieces, heavy, dtype=jnp.bfloat16):
    array = spread * jax.random.normal(key, shape, jnp.float32)
    if pieces:
        array = array * block_levels(key, shape, pieces, -0.22, 0.18)
    return jnp.clip(spiked(array, jax.random.fold_in(key, 3), *heavy), -bound, bound).astype(dtype)


def setup_inputs(seed: int = 0) -> dict:
    splits = jax.random.split(jax.random.key(seed), 6)
    train_gate = bell_draw_with(splits[0], (EXPERTS, D_MODEL, D_EXPERT), D_MODEL ** -0.5, 0.1875, ((0, 4), (1, 8)), (1, 2, 8, 2.0), jnp.float32)
    train_up = bell_draw_with(splits[1], (EXPERTS, D_MODEL, D_EXPERT), D_MODEL ** -0.5, 0.1875, ((0, 4), (1, 8)), (1, 2, 8, 2.0), jnp.float32)
    train_down = bell_draw_with(splits[2], (EXPERTS, D_EXPERT, D_MODEL), D_EXPERT ** -0.5, 0.21875, ((0, 4), (2, 8)), (2, 1, 8, 2.0), jnp.float32)
    router_weight = scatter_about(splits[3], (D_MODEL, EXPERTS), D_MODEL ** -0.5, 0.125, ((0, 8), (1, 4)), jnp.float32)
    router_gain = jnp.clip(1.0 + 0.15 * jax.random.normal(splits[4], (D_MODEL,), jnp.float32), 0.25, 1.75)
    return {"train_gate": train_gate, "train_up": train_up, "train_down": train_down, "router_weight": router_weight, "router_gain": router_gain}


def reference(train_gate, train_up, train_down, router_weight, router_gain):
    scale_gate = jnp.sum(jnp.abs(train_gate), axis=1) / D_MODEL
    ready_gate = (train_gate / jnp.expand_dims(scale_gate, 1)).astype(jnp.bfloat16)
    scale_up = jnp.sum(jnp.abs(train_up), axis=1) / D_MODEL
    ready_up = (train_up / jnp.expand_dims(scale_up, 1)).astype(jnp.bfloat16)
    scale_down = jnp.sum(jnp.abs(train_down), axis=2) / D_MODEL
    ready_down = (train_down / jnp.expand_dims(scale_down, 2)).astype(jnp.bfloat16)
    serve_router = (router_weight * router_gain[:, None]).astype(jnp.bfloat16)
    return ready_gate, ready_up, ready_down, scale_gate, scale_up, scale_down, serve_router
```

```python
import functools

import jax
import jax.numpy as jnp
from jax import lax
from jax.experimental import pallas as pl
from jax.experimental.pallas import tpu as pltpu
from jax.sharding import PartitionSpec as P

VMEM_LIMIT = 60 * 1024 * 1024


def pack_kernel(turn, x_ref, *refs):
    out_ref = refs[-1]
    block = x_ref[0]
    if turn:
        block = block.T
    out_ref[...] = block.reshape(out_ref.shape).astype(jnp.bfloat16)


def pack(train, turn, first, count, carried, at, slots, peers):
    _, rows, columns = train.shape
    outer, inner = (columns, rows) if turn else (rows, columns)
    share = outer // peers
    hbm = pl.BlockSpec(memory_space=pl.ANY)
    return pl.pallas_call(
        functools.partial(pack_kernel, turn),
        grid=(count,),
        in_specs=[pl.BlockSpec((1, rows, columns), lambda e: (first + e, 0, 0))] + [hbm] * len(carried),
        out_specs=pl.BlockSpec((peers, 1, share, inner), lambda e: (0, at + e, 0, 0)),
        out_shape=jax.ShapeDtypeStruct((peers, slots, share, inner), jnp.bfloat16),
        input_output_aliases={1: 0} if carried else {},
        compiler_params=pltpu.CompilerParams(vmem_limit_bytes=VMEM_LIMIT),
        cost_estimate=pl.CostEstimate(
            flops=count * rows * columns, bytes_accessed=count * rows * columns * 6, transcendentals=0
        ),
    )(train, *carried)


def finish_kernel(width, x_ref, *refs):
    ready_ref, scale_ref = refs[-2:]
    peers, _, share, inner = x_ref.shape
    total = jnp.zeros((share, inner), jnp.float32)
    for p in range(peers):
        total += jnp.abs(x_ref[p, 0].astype(jnp.float32))
    scale = jnp.sum(total, axis=1, keepdims=True) / width
    for p in range(peers):
        ready_ref[0, :, p * inner : (p + 1) * inner] = (
            x_ref[p, 0].astype(jnp.float32) / scale
        ).astype(jnp.bfloat16)
    scale_ref[0] = jnp.broadcast_to(scale, (share, 128)).T[0:1]


def finish(received, at, count, carried, first, experts):
    peers, _, share, inner = received.shape
    width = peers * inner
    hbm = pl.BlockSpec(memory_space=pl.ANY)
    return pl.pallas_call(
        functools.partial(finish_kernel, width),
        grid=(count,),
        in_specs=[pl.BlockSpec((peers, 1, share, inner), lambda e: (0, at + e, 0, 0))] + [hbm] * len(carried),
        out_specs=[
            pl.BlockSpec((1, share, width), lambda e: (first + e, 0, 0)),
            pl.BlockSpec((1, 1, share), lambda e: (first + e, 0, 0)),
        ],
        out_shape=[
            jax.ShapeDtypeStruct((experts, share, width), jnp.bfloat16),
            jax.ShapeDtypeStruct((experts, 1, share), jnp.float32),
        ],
        input_output_aliases={1: 0, 2: 1} if carried else {},
        compiler_params=pltpu.CompilerParams(vmem_limit_bytes=VMEM_LIMIT),
        cost_estimate=pl.CostEstimate(
            flops=count * share * width * 4, bytes_accessed=count * share * width * 4, transcendentals=0
        ),
    )(received, *carried)


def shards(ep, fsdp, train_gate, train_up, train_down, router_weight, router_gain):
    experts = train_gate.shape[0]
    part = (router_weight * router_gain[:, None]).astype(jnp.bfloat16).T
    copies = jnp.broadcast_to(part[None], (ep * fsdp,) + part.shape)
    router = lax.all_to_all(copies, ("ep", "fsdp"), split_axis=0, concat_axis=0, tiled=True)

    edge = max(experts * 5 // 16, 1)
    plan = (
        (("down", 0, edge),),
        (("down", edge, experts - edge), ("gate", 0, experts), ("up", 0, experts - edge)),
        (("up", experts - edge, edge),),
    )
    train = {"gate": train_gate, "up": train_up, "down": train_down}
    done = {"gate": (), "up": (), "down": ()}

    def pack_group(group):
        slots, at, packed = sum(count for _, _, count in group), 0, ()
        for name, first, count in group:
            packed = (pack(train[name], name != "down", first, count, packed, at, slots, fsdp),)
            at += count
        return packed[0]

    def finish_group(group, received):
        at = 0
        for name, first, count in group:
            done[name] = finish(received, at, count, done[name], first, experts)
            at += count

    def exchange(packed):
        return lax.all_to_all(packed, "fsdp", split_axis=0, concat_axis=0, tiled=True)

    packed, router = lax.optimization_barrier((pack_group(plan[0]), router))
    received = exchange(packed)
    for last, group in zip(plan, plan[1:]):
        received, packed, done = lax.optimization_barrier((received, pack_group(group), done))
        arrived, received = received, exchange(packed)
        finish_group(last, arrived)
    received, done = lax.optimization_barrier((received, done))
    finish_group(plan[-1], received)

    router = router.reshape((ep, fsdp) + part.shape).transpose(1, 3, 0, 2)
    serve_router = router.reshape(fsdp * part.shape[1], ep * part.shape[0])
    (ready_gate, scale_gate), (ready_up, scale_up), (ready_down, scale_down) = (
        done["gate"],
        done["up"],
        done["down"],
    )
    return (
        jnp.swapaxes(ready_gate, 1, 2),
        jnp.swapaxes(ready_up, 1, 2),
        ready_down,
        scale_gate[:, 0],
        scale_up[:, 0],
        scale_down[:, 0],
        serve_router,
    )


def solution(mesh):
    in_specs = (
        P("ep", "fsdp", None),
        P("ep", "fsdp", None),
        P("ep", None, "fsdp"),
        P("fsdp", "ep"),
        P("fsdp"),
    )
    out_specs = (
        P("ep", None, "fsdp"),
        P("ep", None, "fsdp"),
        P("ep", "fsdp", None),
        P("ep", "fsdp"),
        P("ep", "fsdp"),
        P("ep", "fsdp"),
        P(),
    )
    body = functools.partial(shards, mesh.shape["ep"], mesh.shape["fsdp"])
    return jax.shard_map(body, mesh=mesh, in_specs=in_specs, out_specs=out_specs, check_vma=False)
```
